32 devices in a mesh: dp: 2 (over x), mx: 4 (over y, core), my: 4 (over z).
Axes of the slice: x: 2, y: 2, z: 4, core: 2. Of those that a mesh axis runs over, the one named last changes fastest.
Arguments:
- mentor_final_states: bfloat16 [128, 4608], P('dp'), may hold values from -12 to 12
- mentor_output_matrix: bfloat16 [4608, 4096], P(None, ('mx', 'my')), may hold values from -0.09375 to 0.09375
- learner_final_states: bfloat16 [128, 3584], P('dp', 'mx'), may hold values from -12 to 12
- learner_output_matrix: bfloat16 [3584, 4096], P('mx', 'my'), may hold values from -0.09375 to 0.09375
- loss_mask: int32 [128], P('dp'), may hold values 0 or 1
Outputs:
- mismatch_per_piece: float32 [128], P('dp')
- mean_loss: float32 [], replicated
- student_grad: float32 [128, 4096], P('dp', 'my')
The draws below stay inside these ranges and needn't reach their ends.
All inputs are finite; a program needn't handle non-finite values.
Results may differ from the reference program's by a relative error of at most 0.0003.
Values sent between devices are 32-bit elements.
A program may use at most 64 MiB of HBM per device.

```python
import jax
import jax.numpy as jnp

D_T = 4608
D_S = 3584
WORD_LEXICON = 4096
WINDOW_PIECES = 128


def with_ends(array, key, least, high):
    dims = array.shape
    place = [jax.random.randint(jax.random.fold_in(key, axis), (), 0, dims[axis]) for axis in range(len(dims))]
    array = array.at[tuple(place)].set(least)
    longest = dims.index(max(dims))
    place[longest] = (place[longest] + 1) % dims[longest]
    return array.at[tuple(place)].set(high)


def steps_of(own_key, shape, pieces, smallest, largest):
    def one(dim, shards_of):
        draws = jax.random.uniform(jax.random.fold_in(jax.random.fold_in(own_key, 6), dim), (shards_of,), jnp.float32, smallest / len(pieces), largest / len(pieces))
        return jnp.repeat(jnp.exp(draws), shape[dim] // shards_of).reshape((-1,) + (1,) * (len(shape) - dim - 1))

    level = one(*pieces[0])
    for cut in pieces[1:]:
        level = level * one(*cut)
    return level


def bell_draw(own_key, extent, spread, limit, cuts=(), kind=jnp.bfloat16):
    result = spread * jax.random.normal(own_key, extent, jnp.float32)
    if cuts:
        result = result * steps_of(own_key, extent, cuts, -0.22, 0.18)
    return jnp.clip(result, -limit, limit).astype(kind)


def setup_inputs(seed: int = 0) -> dict:
    arg_keys = jax.random.split(jax.random.key(seed), 6)
    mentor_final_states = bell_draw(arg_keys[0], (WINDOW_PIECES, D_T), 2.0, 12.0, ((0, 2),))
    mentor_output_matrix = bell_draw(arg_keys[1], (D_T, WORD_LEXICON), D_T ** -0.5, 0.09375, ((1, 16),))
    learner_final_states = bell_draw(arg_keys[2], (WINDOW_PIECES, D_S), 2.0, 12.0, ((0, 2), (1, 4)))
    learner_output_matrix = bell_draw(arg_keys[3], (D_S, WORD_LEXICON), D_S ** -0.5, 0.09375, ((0, 4), (1, 4)))
    loss_mask = with_ends((jax.random.randint(arg_keys[4], (WINDOW_PIECES,), 0, 4) < 3).astype(jnp.int32), jax.random.fold_in(arg_keys[4], 1), 0, 1)
    return {"mentor_final_states": mentor_final_states, "mentor_output_matrix": mentor_output_matrix, "learner_final_states": learner_final_states, "learner_output_matrix": learner_output_matrix, "loss_mask": loss_mask}


SOFTENING_HEAT = 2.0


def log_softmax_rows(values):
    row_max = jnp.max(values, axis=1, keepdims=True)
    row_sum = jnp.sum(jnp.exp(values - row_max), axis=1, keepdims=True)
    return values - (row_max + jnp.log(row_sum))


def reference(mentor_final_states, mentor_output_matrix, learner_final_states, learner_output_matrix, loss_mask):
    mentor_softened_scores = jnp.dot(mentor_final_states, mentor_output_matrix, preferred_element_type=jnp.float32) / SOFTENING_HEAT
    learner_softened_scores = jnp.dot(learner_final_states, learner_output_matrix, preferred_element_type=jnp.float32) / SOFTENING_HEAT
    mentor_logarithmic_odds = log_softmax_rows(mentor_softened_scores)
    learner_logarithmic_odds = log_softmax_rows(learner_softened_scores)
    mentor_likelihoods = jnp.exp(mentor_logarithmic_odds)
    mismatch_per_piece = SOFTENING_HEAT * SOFTENING_HEAT * jnp.sum(mentor_likelihoods * (mentor_logarithmic_odds - learner_logarithmic_odds), axis=1)
    piece_importance = loss_mask.astype(jnp.float32)
    usable_count = jnp.sum(piece_importance)
    mean_loss = jnp.sum(piece_importance * mismatch_per_piece) / usable_count
    multiplier = piece_importance * (SOFTENING_HEAT * WORD_LEXICON * WINDOW_PIECES) / usable_count
    student_grad = (jnp.exp(learner_logarithmic_odds) - mentor_likelihoods) * multiplier[:, None]
    return mismatch_per_piece, mean_loss, student_grad
```

```python
import functools

import jax
import jax.numpy as jnp
from jax import lax
from jax.experimental import pallas as pl
from jax.experimental.pallas import tpu as pltpu
from jax.sharding import PartitionSpec as P

SOFTENING_HEAT = 2.0
CORES = 2
TEACHER_CHUNKS = 4
MESH = pl.DeviceIdType.MESH


def kernel(
    sizes,
    ts_hbm, tw_hbm, ss_hbm, sw_hbm, mask_ref,
    mism_ref, loss_ref, grad_ref,
    ts, tw, ss, sw,
    t_own, t_all, s_all, a_send, own, a_recv, b_send, b_recv,
    st_send, st_all, cnt_all, los_all,
    ld_sem, tt_sem, ag_send, ag_sem, rs_send, rs_sem, bs_send, bs_sem,
    st_ssem, st_rsem, cn_ssem, cn_rsem, lo_ssem, lo_rsem,
):
    n_dp, n_mx, n_my = sizes
    h = n_mx // CORES
    group = n_mx * n_my
    dp, mx, my = lax.axis_index("dp"), lax.axis_index("mx"), lax.axis_index("my")
    yy, cc = mx // CORES, mx % CORES
    me = mx * n_my + my
    partner = {"mx": yy * CORES + (1 - cc)}
    tokens, bc = t_own.shape
    kc = tw.shape[0] // TEACHER_CHUNKS

    def remote(src, dst, ssem, rsem, dev):
        return pltpu.make_async_remote_copy(
            src_ref=src, dst_ref=dst, send_sem=ssem, recv_sem=rsem, device_id=dev, device_id_type=MESH
        )

    loads = [pltpu.make_async_copy(ts_hbm, ts, ld_sem.at[0])]
    for k in range(TEACHER_CHUNKS):
        rows = pl.ds(k * kc, kc)
        loads.append(pltpu.make_async_copy(tw_hbm.at[rows, :], tw.at[rows, :], ld_sem.at[1 + k]))
    base = 1 + TEACHER_CHUNKS
    loads.append(pltpu.make_async_copy(ss_hbm, ss, ld_sem.at[base]))
    for k in range(n_mx):
        r, core = k % h, (1 - cc if k < h else cc)
        block = ((yy + r) % h) * CORES + core
        cols = pl.ds(pl.multiple_of(block * bc, bc), bc)
        loads.append(pltpu.make_async_copy(sw_hbm.at[:, cols], sw.at[k], ld_sem.at[base + 1 + k]))
    for c in loads:
        c.start()

    barrier = pltpu.get_barrier_semaphore()
    for k in range(1, group):
        peer = (me + k) % group
        pl.semaphore_signal(
            barrier, inc=1, device_id={"mx": peer // n_my, "my": peer % n_my}, device_id_type=MESH
        )
    for k in range(1, n_dp):
        pl.semaphore_signal(barrier, inc=1, device_id={"dp": (dp + k) % n_dp}, device_id_type=MESH)

    mask = mask_ref[...].astype(jnp.float32)
    cnt_all[dp] = jnp.broadcast_to(jnp.sum(mask, axis=1, keepdims=True), cnt_all.shape[1:])

    loads[0].wait()
    acc = jnp.zeros((tokens, bc), jnp.float32)
    for k in range(TEACHER_CHUNKS):
        loads[1 + k].wait()
        rows = slice(k * kc, (k + 1) * kc)
        acc += jnp.dot(ts[:, rows], tw[rows, :], preferred_element_type=jnp.float32)
    t_own[...] = acc * (1.0 / SOFTENING_HEAT)

    pl.semaphore_wait(barrier, group - 1 + n_dp - 1)

    swap = remote(t_own, t_all.at[my], tt_sem.at[0], tt_sem.at[1], {"mx": my, "my": mx})

    @pl.when(mx != my)
    def _():
        swap.start()

    @pl.when(mx == my)
    def _():
        t_all[mx] = t_own[...]

    def dp_copies(buf, ssem, rsem):
        return [
            remote(buf.at[dp], buf.at[dp], ssem.at[k], rsem.at[k], {"dp": (dp + k) % n_dp})
            for k in range(1, n_dp)
        ]

    cnt_copies = dp_copies(cnt_all, cn_ssem, cn_rsem)
    for c in cnt_copies:
        c.start()

    loads[base].wait()
    ra = []
    for k in range(n_mx):
        loads[base + 1 + k].wait()
        part = jnp.dot(ss[...], sw[k], preferred_element_type=jnp.float32)
        if k < h:
            a_send[k] = part
            c = remote(a_send.at[k], a_recv.at[k], rs_send.at[k], rs_sem.at[k], partner)
            c.start()
            ra.append(c)
        else:
            own[k - h] = part

    rb = []
    for r in list(range(1, h)) + [0]:
        ra[r].wait_recv()
        if r:
            b_send[r] = own[r] + a_recv[r]
            c = remote(
                b_send.at[r], b_recv.at[r], bs_send.at[r], bs_sem.at[r],
                {"mx": ((yy + r) % h) * CORES + cc},
            )
            c.start()
            rb.append(c)
    total = own[0] + a_recv[0]
    for r, c in enumerate(rb):
        c.wait_recv()
        total = total + b_recv[r + 1]
    s_blk = total * (1.0 / SOFTENING_HEAT)
    s_all[mx] = s_blk

    def gather(buf, which):
        firsts = [remote(buf.at[mx], buf.at[mx], ag_send.at[which, r], ag_sem.at[which, r],
                         {"mx": ((yy + r) % h) * CORES + cc}) for r in range(1, h)]
        pairs = []
        for r in range(h):
            slot = ((yy - r + h) % h) * CORES + cc
            pairs.append(remote(buf.at[slot], buf.at[slot], ag_send.at[which, h + r],
                                ag_sem.at[which, h + r], partner))
        return firsts, pairs

    s_first, s_pair = gather(s_all, 0)
    t_first, t_pair = gather(t_all, 1)
    for c in s_first:
        c.start()
    s_pair[0].start()

    @pl.when(mx != my)
    def _():
        swap.wait_recv()

    for c in t_first:
        c.start()
    t_pair[0].start()

    t_blk = t_all[mx]
    mt = jnp.max(t_blk, axis=1, keepdims=True)
    ms = jnp.max(s_blk, axis=1, keepdims=True)
    td, sd = t_blk - mt, s_blk - ms
    et = jnp.exp(td)
    st = jnp.sum(et, axis=1, keepdims=True)
    sS = jnp.sum(jnp.exp(sd), axis=1, keepdims=True)
    cr = jnp.sum(et * (td - sd), axis=1, keepdims=True)
    lane = lax.broadcasted_iota(jnp.int32, (tokens, 128), 1)
    packed = jnp.where(lane == 0, mt, jnp.where(lane == 1, st, jnp.where(lane == 2, ms, jnp.where(lane == 3, sS, cr))))
    if tokens < 128:
        packed = jnp.concatenate([packed, jnp.zeros((128 - tokens, 128), jnp.float32)], axis=0)
    tile = packed.T[:8, :]
    st_send[...] = tile
    st_all[me] = tile
    st_copies = []
    for k in range(1, group):
        peer = (me + k) % group
        c = remote(st_send, st_all.at[me], st_ssem.at[k], st_rsem.at[k],
                   {"mx": peer // n_my, "my": peer % n_my})
        c.start()
        st_copies.append(c)

    for firsts, pairs in ((s_first, s_pair), (t_first, t_pair)):
        for r, c in enumerate(firsts):
            c.wait_recv()
            pairs[r + 1].start()

    for c in cnt_copies:
        c.wait_recv()
    count = jnp.sum(cnt_all[:, 0:1, :], axis=0)
    for c in st_copies:
        c.wait_recv()
    mts, sts, mss, sss, crs = (st_all[:, i, :] for i in range(5))
    top_t = jnp.max(mts, axis=0, keepdims=True)
    top_s = jnp.max(mss, axis=0, keepdims=True)
    w = jnp.exp(mts - top_t)
    sum_t = jnp.sum(sts * w, axis=0, keepdims=True)
    sum_s = jnp.sum(sss * jnp.exp(mss - top_s), axis=0, keepdims=True)
    d = jnp.sum(w * (crs + sts * ((mts - top_t) - (mss - top_s))), axis=0, keepdims=True)
    log_t, log_s = jnp.log(sum_t), jnp.log(sum_s)
    mism = (SOFTENING_HEAT * SOFTENING_HEAT) * (d / sum_t - log_t + log_s)
    mism = mism[:, :tokens]
    mism_ref[...] = mism
    los_all[dp] = jnp.broadcast_to(jnp.sum(mask * mism, axis=1, keepdims=True), los_all.shape[1:])
    los_copies = dp_copies(los_all, lo_ssem, lo_rsem)
    for c in los_copies:
        c.start()

    multiplier = SOFTENING_HEAT * n_mx * n_my * bc * n_dp * tokens
    mult = mask * multiplier / count[:, :tokens]
    if tokens < 128:
        mult = jnp.concatenate([mult, jnp.zeros((1, 128 - tokens), jnp.float32)], axis=1)
    row = lax.broadcasted_iota(jnp.int32, (128, 128), 0)
    back = jnp.where(row == 0, top_t + log_t, jnp.where(row == 1, top_s + log_s, mult)).T
    lt, ls, mu = back[:tokens, 0:1], back[:tokens, 1:2], back[:tokens, 2:3]

    for c in s_pair + t_pair:
        c.wait_recv()
    for j in range(n_mx):
        grad_ref[:, j * bc:(j + 1) * bc] = (jnp.exp(s_all[j] - ls) - jnp.exp(t_all[j] - lt)) * mu

    for c in los_copies:
        c.wait_recv()
    loss_ref[...] = jnp.sum(los_all[:, 0:1, 0:1], axis=0) / count[:, 0:1]

    @pl.when(mx != my)
    def _():
        swap.wait_send()

    for c in cnt_copies + los_copies + ra + rb + s_first + s_pair + t_first + t_pair + st_copies:
        c.wait_send()


def shards(sizes, ts, tw, ss, sw, mask):
    n_dp, n_mx, n_my = sizes
    tokens, bc = ts.shape[0], tw.shape[1]
    cols = sw.shape[1]
    h = n_mx // CORES
    group = n_mx * n_my
    f32 = jnp.float32
    V, D = pltpu.VMEM, pltpu.SemaphoreType.DMA
    hbm = pl.BlockSpec(memory_space=pltpu.HBM)
    vm = pl.BlockSpec(memory_space=pltpu.VMEM)
    mism, loss, grad = pl.pallas_call(
        functools.partial(kernel, sizes),
        out_shape=(
            jax.ShapeDtypeStruct((1, tokens), f32),
            jax.ShapeDtypeStruct((1, 1), f32),
            jax.ShapeDtypeStruct((tokens, cols), f32),
        ),
        in_specs=[hbm, hbm, hbm, hbm, vm],
        out_specs=(vm, vm, vm),
        scratch_shapes=[
            V(ts.shape, ts.dtype), V(tw.shape, tw.dtype), V(ss.shape, ss.dtype),
            V((n_mx, sw.shape[0], bc), sw.dtype),
            V((tokens, bc), f32), V((n_mx, tokens, bc), f32), V((n_mx, tokens, bc), f32),
            V((h, tokens, bc), f32), V((h, tokens, bc), f32), V((h, tokens, bc), f32),
            V((h, tokens, bc), f32), V((h, tokens, bc), f32),
            V((8, 128), f32), V((group, 8, 128), f32), V((n_dp, 8, 128), f32), V((n_dp, 8, 128), f32),
            D((2 + TEACHER_CHUNKS + n_mx,)), D((2,)),
            D((2, 2 * h)), D((2, 2 * h)), D((h,)), D((h,)), D((h,)), D((h,)),
            D((group,)), D((group,)), D((n_dp,)), D((n_dp,)), D((n_dp,)), D((n_dp,)),
        ],
        compiler_params=pltpu.CompilerParams(
            collective_id=0, has_side_effects=True, vmem_limit_bytes=66_500_000
        ),
    )(ts, tw, ss, sw, mask.reshape(1, tokens))
    return mism.reshape(tokens), loss.reshape(()), grad


def solution(mesh):
    sizes = (mesh.shape["dp"], mesh.shape["mx"], mesh.shape["my"])
    placed = (P("dp", None), P(None, ("mx", "my")), P("dp", "mx"), P("mx", "my"), P("dp"))
    return jax.shard_map(
        functools.partial(shards, sizes), mesh=mesh, in_specs=placed,
        out_specs=(P("dp"), P(), P("dp", "my")), check_vma=False,
    )
```

```python
import functools

import jax
import jax.numpy as jnp
from jax import lax
from jax.experimental import pallas as pl
from jax.experimental.pallas import tpu as pltpu
from jax.sharding import PartitionSpec as P

SOFTENING_HEAT = 2.0
CORES = 2
TEACHER_CHUNKS = 4
MESH = pl.DeviceIdType.MESH


def kernel(
    sizes,
    ts_hbm, tw_hbm, ss_hbm, sw_hbm, mask_ref,
    small_ref, grad_ref,
    ts, tw, ss, sw,
    t_own, t_all, s_all, a_send, own, a_recv, b_send, b_recv,
    st_send, st_all, cnt_all, los_all,
    ld_sem, tt_sem, ag_send, ag_sem, rs_send, rs_sem, bs_send, bs_sem,
    st_ssem, st_rsem, cn_ssem, cn_rsem, lo_ssem, lo_rsem,
):
    n_dp, n_mx, n_my = sizes
    h = n_mx // CORES
    group = n_mx * n_my
    dp, mx, my = lax.axis_index("dp"), lax.axis_index("mx"), lax.axis_index("my")
    yy, cc = mx // CORES, mx % CORES
    me = mx * n_my + my
    partner = {"mx": yy * CORES + (1 - cc)}
    tokens, bc = t_own.shape
    kc = tw.shape[0] // TEACHER_CHUNKS

    def remote(src, dst, ssem, rsem, dev):
        return pltpu.make_async_remote_copy(
            src_ref=src, dst_ref=dst, send_sem=ssem, recv_sem=rsem, device_id=dev, device_id_type=MESH
        )

    loads = [pltpu.make_async_copy(ts_hbm, ts, ld_sem.at[0])]
    for k in range(TEACHER_CHUNKS):
        rows = pl.ds(k * kc, kc)
        loads.append(pltpu.make_async_copy(tw_hbm.at[rows, :], tw.at[rows, :], ld_sem.at[1 + k]))
    base = 1 + TEACHER_CHUNKS
    loads.append(pltpu.make_async_copy(ss_hbm, ss, ld_sem.at[base]))
    for k in range(n_mx):
        r, core = k % h, (1 - cc if k < h else cc)
        block = ((yy + r) % h) * CORES + core
        cols = pl.ds(pl.multiple_of(block * bc, bc), bc)
        loads.append(pltpu.make_async_copy(sw_hbm.at[:, cols], sw.at[k], ld_sem.at[base + 1 + k]))
    for c in loads[:base]:
        c.start()

    barrier = pltpu.get_barrier_semaphore()
    for k in range(1, group):
        peer = (me + k) % group
        pl.semaphore_signal(
            barrier, inc=1, device_id={"mx": peer // n_my, "my": peer % n_my}, device_id_type=MESH
        )
    for k in range(1, n_dp):
        pl.semaphore_signal(barrier, inc=1, device_id={"dp": (dp + k) % n_dp}, device_id_type=MESH)

    mask = mask_ref[...].astype(jnp.float32)
    cnt_all[dp] = jnp.broadcast_to(jnp.sum(mask, axis=1, keepdims=True), cnt_all.shape[1:])

    loads[0].wait()
    acc = jnp.zeros((tokens, bc), jnp.float32)
    for k in range(TEACHER_CHUNKS):
        loads[1 + k].wait()
        if k == 1:
            for c in loads[base:]:
                c.start()
        rows = slice(k * kc, (k + 1) * kc)
        acc += jnp.dot(ts[:, rows], tw[rows, :], preferred_element_type=jnp.float32)
    t_own[...] = acc * (1.0 / SOFTENING_HEAT)

    pl.semaphore_wait(barrier, group - 1 + n_dp - 1)

    swap = remote(t_own, t_all.at[my], tt_sem.at[0], tt_sem.at[1], {"mx": my, "my": mx})

    @pl.when(mx != my)
    def _():
        swap.start()

    @pl.when(mx == my)
    def _():
        t_all[mx] = t_own[...]

    def dp_copies(buf, ssem, rsem):
        return [
            remote(buf.at[dp], buf.at[dp], ssem.at[k], rsem.at[k], {"dp": (dp + k) % n_dp})
            for k in range(1, n_dp)
        ]

    cnt_copies = dp_copies(cnt_all, cn_ssem, cn_rsem)
    for c in cnt_copies:
        c.start()

    loads[base].wait()
    ra = []
    for k in range(n_mx):
        loads[base + 1 + k].wait()
        part = jnp.dot(ss[...], sw[k], preferred_element_type=jnp.float32)
        if k < h:
            a_send[k] = part
            c = remote(a_send.at[k], a_recv.at[k], rs_send.at[k], rs_sem.at[k], partner)
            c.start()
            ra.append(c)
        else:
            own[k - h] = part

    rb = []
    for r in list(range(1, h)) + [0]:
        ra[r].wait_recv()
        if r:
            b_send[r] = own[r] + a_recv[r]
            c = remote(
                b_send.at[r], b_recv.at[r], bs_send.at[r], bs_sem.at[r],
                {"mx": ((yy + r) % h) * CORES + cc},
            )
            c.start()
            rb.append(c)
    total = own[0] + a_recv[0]
    for r, c in enumerate(rb):
        c.wait_recv()
        total = total + b_recv[r + 1]
    s_blk = total * (1.0 / SOFTENING_HEAT)
    s_all[mx] = s_blk

    def gather(buf, which):
        firsts = [remote(buf.at[mx], buf.at[mx], ag_send.at[which, r], ag_sem.at[which, r],
                         {"mx": ((yy + r) % h) * CORES + cc}) for r in range(1, h)]
        pairs = []
        for r in range(h):
            slot = ((yy - r + h) % h) * CORES + cc
            pairs.append(remote(buf.at[slot], buf.at[slot], ag_send.at[which, h + r],
                                ag_sem.at[which, h + r], partner))
        return firsts, pairs

    s_first, s_pair = gather(s_all, 0)
    t_first, t_pair = gather(t_all, 1)
    for c in s_first:
        c.start()
    s_pair[0].start()

    @pl.when(mx != my)
    def _():
        swap.wait_recv()

    for c in t_first:
        c.start()
    t_pair[0].start()

    t_blk = t_all[mx]
    mt = jnp.max(t_blk, axis=1, keepdims=True)
    ms = jnp.max(s_blk, axis=1, keepdims=True)
    td, sd = t_blk - mt, s_blk - ms
    et = jnp.exp(td)
    st = jnp.sum(et, axis=1, keepdims=True)
    sS = jnp.sum(jnp.exp(sd), axis=1, keepdims=True)
    cr = jnp.sum(et * (td - sd), axis=1, keepdims=True)
    lane = lax.broadcasted_iota(jnp.int32, (tokens, 128), 1)
    packed = jnp.where(lane == 0, mt, jnp.where(lane == 1, st, jnp.where(lane == 2, ms, jnp.where(lane == 3, sS, cr))))
    if tokens < 128:
        packed = jnp.concatenate([packed, jnp.zeros((128 - tokens, 128), jnp.float32)], axis=0)
    tile = packed.T[:8, :]
    st_send[...] = tile
    st_all[me] = tile
    st_copies = []
    for k in range(1, group):
        peer = (me + k) % group
        c = remote(st_send, st_all.at[me], st_ssem.at[k], st_rsem.at[k],
                   {"mx": peer // n_my, "my": peer % n_my})
        c.start()
        st_copies.append(c)

    for firsts, pairs in ((s_first, s_pair), (t_first, t_pair)):
        for r, c in enumerate(firsts):
            c.wait_recv()
            pairs[r + 1].start()

    for c in cnt_copies:
        c.wait_recv()
    count = jnp.sum(cnt_all[:, 0:1, :], axis=0)
    for c in st_copies:
        c.wait_recv()
    mts, sts, mss, sss, crs = (st_all[:, i, :] for i in range(5))
    top_t = jnp.max(mts, axis=0, keepdims=True)
    top_s = jnp.max(mss, axis=0, keepdims=True)
    w = jnp.exp(mts - top_t)
    sum_t = jnp.sum(sts * w, axis=0, keepdims=True)
    sum_s = jnp.sum(sss * jnp.exp(mss - top_s), axis=0, keepdims=True)
    d = jnp.sum(w * (crs + sts * ((mts - top_t) - (mss - top_s))), axis=0, keepdims=True)
    log_t, log_s = jnp.log(sum_t), jnp.log(sum_s)
    mism = (SOFTENING_HEAT * SOFTENING_HEAT) * (d / sum_t - log_t + log_s)
    mism = mism[:, :tokens]
    small_ref[0:1, :tokens] = mism
    los_all[dp] = jnp.broadcast_to(jnp.sum(mask * mism, axis=1, keepdims=True), los_all.shape[1:])
    los_copies = dp_copies(los_all, lo_ssem, lo_rsem)
    for c in los_copies:
        c.start()

    multiplier = SOFTENING_HEAT * n_mx * n_my * bc * n_dp * tokens
    mult = mask * multiplier / count[:, :tokens]
    if tokens < 128:
        mult = jnp.concatenate([mult, jnp.zeros((1, 128 - tokens), jnp.float32)], axis=1)
    row = lax.broadcasted_iota(jnp.int32, (128, 128), 0)
    back = jnp.where(row == 0, top_t + log_t, jnp.where(row == 1, top_s + log_s, mult)).T
    lt, ls, mu = back[:tokens, 0:1], back[:tokens, 1:2], back[:tokens, 2:3]

    for c in s_pair + t_pair:
        c.wait_recv()
    for j in range(n_mx):
        grad_ref[:, j * bc:(j + 1) * bc] = (jnp.exp(s_all[j] - ls) - jnp.exp(t_all[j] - lt)) * mu

    for c in los_copies:
        c.wait_recv()
    small_ref[1:2, :] = jnp.sum(los_all[:, 0:1, :], axis=0) / count

    @pl.when(mx != my)
    def _():
        swap.wait_send()

    for c in cnt_copies + los_copies + ra + rb + s_first + s_pair + t_first + t_pair + st_copies:
        c.wait_send()


def deliver(small_ref, grad_ref, mism_ref, loss_ref, out_ref, sem):
    copy = pltpu.make_async_copy(grad_ref, out_ref, sem)
    copy.start()
    mism_ref[...] = small_ref[0:1, :mism_ref.shape[1]]
    loss_ref[...] = small_ref[1:2, 0:1]
    copy.wait()


def shards(sizes, ts, tw, ss, sw, mask):
    n_dp, n_mx, n_my = sizes
    tokens, bc = ts.shape[0], tw.shape[1]
    cols = sw.shape[1]
    h = n_mx // CORES
    group = n_mx * n_my
    f32 = jnp.float32
    V, D = pltpu.VMEM, pltpu.SemaphoreType.DMA
    hbm = pl.BlockSpec(memory_space=pltpu.HBM)
    vm = pl.BlockSpec(memory_space=pltpu.VMEM)
    small, grad = pl.pallas_call(
        functools.partial(kernel, sizes),
        out_shape=(
            V((8, max(tokens, 128)), f32),
            V((tokens, cols), f32),
        ),
        in_specs=[hbm, hbm, hbm, hbm, vm],
        out_specs=(vm, vm),
        scratch_shapes=[
            V(ts.shape, ts.dtype), V(tw.shape, tw.dtype), V(ss.shape, ss.dtype),
            V((n_mx, sw.shape[0], bc), sw.dtype),
            V((tokens, bc), f32), V((n_mx, tokens, bc), f32), V((n_mx, tokens, bc), f32),
            V((h, tokens, bc), f32), V((h, tokens, bc), f32), V((h, tokens, bc), f32),
            V((h, tokens, bc), f32), V((h, tokens, bc), f32),
            V((8, 128), f32), V((group, 8, 128), f32), V((n_dp, 8, 128), f32), V((n_dp, 8, 128), f32),
            D((2 + TEACHER_CHUNKS + n_mx,)), D((2,)),
            D((2, 2 * h)), D((2, 2 * h)), D((h,)), D((h,)), D((h,)), D((h,)),
            D((group,)), D((group,)), D((n_dp,)), D((n_dp,)), D((n_dp,)), D((n_dp,)),
        ],
        compiler_params=pltpu.CompilerParams(
            collective_id=0, has_side_effects=True, vmem_limit_bytes=64_000_000
        ),
    )(ts, tw, ss, sw, mask.reshape(1, tokens))
    mism, loss, grad = pl.pallas_call(
        deliver,
        out_shape=(
            jax.ShapeDtypeStruct((1, tokens), f32),
            jax.ShapeDtypeStruct((1, 1), f32),
            jax.ShapeDtypeStruct((tokens, cols), f32),
        ),
        in_specs=[vm, vm],
        out_specs=(vm, vm, hbm),
        scratch_shapes=[D],
        compiler_params=pltpu.CompilerParams(vmem_limit_bytes=16 * 1024 * 1024),
    )(
        pltpu.with_memory_space_constraint(small, pltpu.VMEM),
        pltpu.with_memory_space_constraint(grad, pltpu.VMEM),
    )
    return mism.reshape(tokens), loss.reshape(()), grad


def solution(mesh):
    sizes = (mesh.shape["dp"], mesh.shape["mx"], mesh.shape["my"])
    placed = (P("dp", None), P(None, ("mx", "my")), P("dp", "mx"), P("mx", "my"), P("dp"))
    return jax.shard_map(
        functools.partial(shards, sizes), mesh=mesh, in_specs=placed,
        out_specs=(P("dp"), P(), P("dp", "my")), check_vma=False,
    )
```
